128 devices in a mesh: obs: 4 (over z), face: 32 (over x, y, core).
Axes of the slice: x: 4, y: 4, z: 4, core: 2. Of those that a mesh axis runs over, the one named last changes fastest.
Arguments:
- density: float32 [34, 32768], P(None, ('obs', 'face')), may hold values from 0.6 to 1.4
- velocity: float32 [3, 34, 32768], P(None, None, ('obs', 'face')), may hold values from -6 to 6
- pressure: float32 [34, 32768], P(None, ('obs', 'face')), may hold values from -6 to 6
- normal: float32 [3, 32768], P(None, ('obs', 'face')), may hold values from -1 to 1, as said below
- direction: float32 [128, 32, 3], P(('obs', 'face')), may hold values from -1 to 1, as said below
- weights: bfloat16 [128, 32, 768, 256], P(('obs', 'face')), may hold values from -0.21875 to 0.21875
- bin_index: int32 [128, 32], P(('obs', 'face')), may hold values from 0 to 31, as said below
- group_index: int32 [128, 32], P(('obs', 'face')), may hold values from 0 to 3
- item_count: int32 [128], P(('obs', 'face')), may hold values from 16 to 32, as said below
Outputs:
- signal: float32 [1024, 1024], P('face', 'obs')
The draws below stay inside these ranges and needn't reach their ends.
Inputs may be any that keep to these rules, and one draw needn't show every extreme that they name: `bin_index`: no time block is named more than 2 times in one device's list; in every draw some device names a block 2 times among its live entries. `item_count`: some device has all 32 entries live. Each face's normal has unit length. Each entry's direction has unit length.
All inputs are finite; a program needn't handle non-finite values.
Results may differ from the reference program's by a relative error of at most 0.0029.
Values sent between devices are 32-bit elements; how exact they have to be, the bound alone decides.
A program may use at most 64 MiB of HBM per device.

```python
import math
import jax
import jax.numpy as jnp
from jax import lax

FACE_DEV = 256
OBS_GROUP = 256
WINDOW_STEPS = 32
SLOT_CAP = 2
LIST_LEN = 32
TOTAL_FACES = 32768
OBSERVERS = 1024
SAMPLES = 1024
DEVICES = 128


def unit_vectors(key, count):
    first, second = jax.random.split(key)
    height = jax.random.uniform(first, (count,), jnp.float32, -1.0, 1.0)
    azimuth = jax.random.uniform(second, (count,), jnp.float32, -math.pi, math.pi)
    radius = jnp.sqrt(jnp.maximum(1.0 - height * height, 0.0))
    return (radius * jnp.cos(azimuth), radius * jnp.sin(azimuth), height)


def draw_normal(key, part):
    east, north, upward = unit_vectors(jax.random.fold_in(key, 11), TOTAL_FACES)
    return jnp.stack([east, north, upward], axis=0).astype(jnp.float32)


def draw_direction(key, part):
    devices = TOTAL_FACES // FACE_DEV
    east, north, upward = unit_vectors(jax.random.fold_in(key, 12), devices * LIST_LEN)
    return jnp.stack([east, north, upward], axis=-1).reshape(devices, LIST_LEN, 3).astype(jnp.float32)


def draw_bin_index(key, part):
    devices = TOTAL_FACES // FACE_DEV
    n_blocks = SAMPLES // WINDOW_STEPS

    def one_row(row_key):
        order_key, block_key = jax.random.split(row_key)
        order = jax.random.permutation(order_key, LIST_LEN)
        blocks = jax.random.permutation(block_key, n_blocks)
        return blocks[order // SLOT_CAP].astype(jnp.int32)
    return jax.vmap(one_row)(jax.random.split(jax.random.fold_in(key, 13), devices))


def draw_item_count(key, part):
    devices = TOTAL_FACES // FACE_DEV
    first, second, third = jax.random.split(jax.random.fold_in(key, 14), 3)
    base = jax.random.randint(first, (devices,), LIST_LEN // 2, LIST_LEN + 1)
    full = jax.random.randint(second, (devices,), 0, 8) == 0
    chosen = jax.random.randint(third, (), 0, devices)
    forced = jnp.arange(devices) == chosen
    return jnp.where(full | forced, LIST_LEN, jnp.minimum(base, LIST_LEN)).astype(jnp.int32)


def plant(array, rng, low, top_value):
    longest = array.shape.index(max(array.shape))
    spots = []
    for shift in (0, 1):
        where = [jax.random.randint(jax.random.fold_in(rng, axis), (), 0, length) for axis, length in enumerate(array.shape)]
        where[longest] = (where[longest] + shift) % array.shape[longest]
        spots.append(tuple(where))
    return array.at[spots[0]].set(low).at[spots[1]].set(top_value)


def steps_of(key, shape, cuts, smallest, high):
    level, own = 1.0, jax.random.fold_in(key, 6)
    for axis_at, parts in cuts:
        draws = jnp.exp(jax.random.uniform(jax.random.fold_in(own, axis_at), (parts,), jnp.float32, smallest / len(cuts), high / len(cuts)))
        level = level * jnp.repeat(draws, shape[axis_at] // parts).reshape([-1 if axis == axis_at else 1 for axis in range(len(shape))])
    return level


def bell_draw(own_key, extent, width, bound, cuts=(), kind=jnp.bfloat16):
    loudness = steps_of(own_key, extent, cuts, -0.22, 0.18) if cuts else 1.0
    result = jax.random.normal(own_key, extent, jnp.float32) * width * loudness
    return jnp.minimum(jnp.maximum(result, -bound), bound).astype(kind)


def setup_inputs(seed: int = 0) -> dict:
    splits = jax.random.split(jax.random.key(seed), 10)
    density = jnp.clip(0.6 + 0.79999995 * jax.random.uniform(splits[0], (WINDOW_STEPS + 2, TOTAL_FACES), jnp.float32) ** steps_of(splits[0], (WINDOW_STEPS + 2, TOTAL_FACES), ((1, 128),), -0.2, 0.2), 0.6, 1.4)
    velocity = bell_draw(splits[1], (3, WINDOW_STEPS + 2, TOTAL_FACES), 1.0, 6.0, ((2, 128),), jnp.float32)
    pressure = bell_draw(splits[2], (WINDOW_STEPS + 2, TOTAL_FACES), 1.0, 6.0, ((1, 128),), jnp.float32)
    normal = draw_normal(jax.random.fold_in(splits[9], 71), 0)
    direction = draw_direction(jax.random.fold_in(splits[9], 71), 0)
    weights = bell_draw(splits[5], (DEVICES, LIST_LEN, 3 * FACE_DEV, OBS_GROUP), (3 * FACE_DEV) ** -0.5, 0.21875, ((0, 128),))
    bin_index = draw_bin_index(jax.random.fold_in(splits[9], 71), 0)
    group_index = plant(jax.random.randint(splits[7], (DEVICES, LIST_LEN), 0, OBSERVERS // OBS_GROUP), jax.random.fold_in(splits[7], 1), 0, (OBSERVERS // OBS_GROUP) - 1).astype(jnp.int32)
    item_count = draw_item_count(jax.random.fold_in(splits[9], 71), 0)
    return dict(density=density, velocity=velocity, pressure=pressure, normal=normal, direction=direction, weights=weights, bin_index=bin_index, group_index=group_index, item_count=item_count)


def face_terms(dens, veloc, press, norms):
    normal_speed = veloc[0] * norms[0][None] + veloc[1] * norms[1][None] + veloc[2] * norms[2][None]
    flux = dens * normal_speed
    load_first = press * norms[0][None] + dens * veloc[0] * normal_speed
    load_second = press * norms[1][None] + dens * veloc[1] * normal_speed
    load_third = press * norms[2][None] + dens * veloc[2] * normal_speed
    thick = 0.5 * (flux[2:] - flux[:-2])
    return thick, load_first, load_second, load_third


def item_source(thick, load_first, load_second, load_third, heading):
    radial = heading[0] * load_first + heading[1] * load_second + heading[2] * load_third
    rate = 0.5 * (radial[2:] - radial[:-2])
    return jnp.concatenate([thick, rate, radial[1:-1]], axis=1).astype(jnp.bfloat16)


def reference(density, velocity, pressure, normal, direction, weights, bin_index, group_index, item_count):
    n_devices = weights.shape[0]
    per_device = density.shape[1] // n_devices
    rows = density.shape[0]
    dens_dev = density.reshape(rows, n_devices, per_device).transpose(1, 0, 2)
    press_dev = pressure.reshape(rows, n_devices, per_device).transpose(1, 0, 2)
    veloc_dev = velocity.reshape(3, rows, n_devices, per_device).transpose(2, 0, 1, 3)
    norms_dev = normal.reshape(3, n_devices, per_device).transpose(1, 0, 2)
    n_blocks = SAMPLES // WINDOW_STEPS
    n_groups = OBSERVERS // OBS_GROUP
    start = jnp.zeros((n_blocks, n_groups, WINDOW_STEPS, OBS_GROUP), jnp.float32)

    def device_step(signal, inputs):
        dens, veloc, press, norms, headings, matrices, blocks_of, groups_of, live_count = inputs
        thick, load_first, load_second, load_third = face_terms(dens, veloc, press, norms)
        for listed in range(LIST_LEN):
            source = item_source(thick, load_first, load_second, load_third, headings[listed])
            block = jnp.dot(source, matrices[listed], preferred_element_type=jnp.float32)
            switch = (listed < live_count).astype(jnp.float32)
            signal = signal.at[blocks_of[listed], groups_of[listed]].add(block * switch)
        return signal, None

    signal, _ = lax.scan(device_step, start, (dens_dev, veloc_dev, press_dev, norms_dev, direction, weights, bin_index, group_index, item_count))
    return signal.transpose(0, 2, 1, 3).reshape(SAMPLES, OBSERVERS)
```

```python
import functools

import jax
import jax.numpy as jnp
from jax import lax
from jax.experimental import pallas as pl
from jax.experimental.pallas import tpu as pltpu
from jax.sharding import PartitionSpec as P

ITEMS = 32
STEPS = 32
FACES = 256
HALF = 128
CHUNK = 4
CHUNKS = ITEMS // CHUNK
EMPTY = ITEMS

X, Y, Z = 0, 1, 2
PATHS = (
    (X, Z, Y),
    (Y, Z, X),
    (Z, X, Y),
    (X, Z, Y),
    (X, Z, Y),
    (Y, Z, X),
    (Z, Y, X),
    (Y, Z, X),
)
ORDER = (
    (1, 1), (2, 1), (0, 1), (5, 1), (6, 1), (3, 1),
    (1, 2), (2, 2), (0, 2), (4, 1), (7, 1), (3, 2), (6, 2), (5, 2),
    (1, 3), (2, 3), (0, 3), (4, 2), (7, 2), (3, 3), (6, 3), (5, 3),
    (1, 4), (2, 4), (0, 4), (4, 3), (7, 3), (3, 4), (6, 4), (5, 4),
    (4, 4), (7, 4),
)


def kernel(
    dens_hbm, veloc_hbm, press_hbm, norm_hbm, head_hbm, weight_hbm, bin_hbm, group_hbm, count_hbm,
    out_ref,
    dens, veloc, press, norms, head, bins, groups, count,
    faces, terms, thick, sources, matrices, own_first, own_second, other_first, other_second, table, table_there, look, look_there,
    acc, first_in, second_in, third_in,
    input_sem, matrix_sem, look_sem, send_sem, recv_sem,
):
    obs = lax.axis_index("obs")
    face = lax.axis_index("face")
    core = lax.rem(face, 2)
    chip = face // 2
    here = (chip // 4, lax.rem(chip, 4), obs)

    def at(axis, step):
        place = list(here)
        place[axis] = lax.rem(here[axis] + step, 4)
        return (place[2], (place[0] * 4 + place[1]) * 2 + core)

    partner = (obs, chip * 2 + (1 - core))
    own, other = (own_first, own_second), (other_first, other_second)

    inputs = [
        pltpu.make_async_copy(source, target, input_sem.at[place])
        for place, (source, target) in enumerate(
            (
                (bin_hbm, bins),
                (group_hbm, groups),
                (count_hbm, count),
                (head_hbm, head),
                (dens_hbm, dens),
                (veloc_hbm, veloc),
                (press_hbm, press),
                (norm_hbm, norms),
            )
        )
    ]
    for copy in inputs:
        copy.start()

    def matrix_copy(half, chunk):
        return pltpu.make_async_copy(
            weight_hbm.at[pl.ds(chunk * CHUNK, CHUNK), :, pl.ds(half * HALF, HALF)],
            matrices.at[half, pl.ds(chunk * CHUNK, CHUNK)],
            matrix_sem.at[half * CHUNKS + chunk],
        )

    for half in range(2):
        for chunk in range(CHUNKS):
            matrix_copy(half, chunk).start()

    barrier = pltpu.get_barrier_semaphore()
    greeted = [partner] + [at(axis, step) for axis in range(3) for step in (1, 2, 3)]
    for device in greeted:
        pl.semaphore_signal(
            barrier, inc=1, device_id=device, device_id_type=pl.DeviceIdType.MESH
        )

    sent = []

    def send(source, target, device):
        place = len(sent)
        copy = pltpu.make_async_remote_copy(
            src_ref=source,
            dst_ref=target,
            send_sem=send_sem.at[place],
            recv_sem=recv_sem.at[place],
            device_id=device,
            device_id_type=pl.DeviceIdType.MESH,
        )
        copy.start()
        sent.append(copy)
        return copy

    for half in range(2):
        own[half][EMPTY] = jnp.zeros((STEPS, HALF), jnp.float32)
        other[half][EMPTY] = jnp.zeros((STEPS, HALF), jnp.float32)

    for copy in inputs[:3]:
        copy.wait()
    rows = lax.broadcasted_iota(jnp.int32, (ITEMS, ITEMS), 0)
    columns = lax.broadcasted_iota(jnp.int32, (ITEMS, ITEMS), 1)
    codes = jnp.broadcast_to(bins[...] * 4 + groups[...], (ITEMS, ITEMS))
    code = jnp.sum(jnp.where(rows == columns, codes, 0), axis=1, keepdims=True)
    entry = lax.broadcasted_iota(jnp.int32, (ITEMS, 128), 0)
    place = lax.broadcasted_iota(jnp.int32, (ITEMS, 128), 1)
    match = (jnp.broadcast_to(code, (ITEMS, 128)) == place) & (entry < count[0, 0])
    low = jnp.min(jnp.where(match, entry, EMPTY), axis=0, keepdims=True)
    high = jnp.max(jnp.where(match, entry, -1), axis=0, keepdims=True)
    table[0:1, :] = low
    table[1:2, :] = jnp.where(high > low, high, EMPTY)

    for copy in inputs[3:]:
        copy.wait()
    normal = [norms[c : c + 1, :] for c in range(3)]
    speed = veloc[0] * normal[0] + veloc[1] * normal[1] + veloc[2] * normal[2]
    faces[3] = dens[...] * speed
    for c in range(3):
        faces[c] = press[...] * normal[c] + dens[...] * veloc[c] * speed
    for c in range(3):
        terms[c] = 0.5 * (faces[c, 2:34, :] - faces[c, 0:32, :])
        terms[3 + c] = faces[c, 1:33, :]
    thick[...] = (0.5 * (faces[3, 2:34, :] - faces[3, 0:32, :])).astype(jnp.bfloat16)

    def blocks(half, chunk):
        matrix_copy(half, chunk).wait()
        for item in range(chunk * CHUNK, (chunk + 1) * CHUNK):
            if half == 0:
                d0, d1, d2 = head[0, 0, item], head[1, 0, item], head[2, 0, item]
                rate = d0 * terms[0] + d1 * terms[1] + d2 * terms[2]
                radial = d0 * terms[3] + d1 * terms[4] + d2 * terms[5]
                source = jnp.concatenate(
                    [thick[...], rate.astype(jnp.bfloat16), radial.astype(jnp.bfloat16)], axis=1
                )
                sources[item] = source
            else:
                source = sources[item]
            own[half][item] = jnp.dot(
                source, matrices[half, item], preferred_element_type=jnp.float32
            )

    def pass_on(half, chunk):
        part = pl.ds(chunk * CHUNK, CHUNK)
        return send(own[half].at[part], other[half].at[part], partner)

    def assemble(half):
        for rx in range(4):
            for ry in range(4):
                for rz in range(4):
                    gx = lax.rem(here[0] + rx, 4)
                    gy = lax.rem(here[1] + ry, 4)
                    gz = lax.rem(here[2] + rz, 4)
                    where = ((gx * 4 + gy) * 2 + core) * 4 + gz
                    total = (
                        own[half][look[0, where]]
                        + own[half][look[1, where]]
                        + other[half][look_there[0, where]]
                        + other[half][look_there[1, where]]
                    )
                    for row in range(4):
                        tile = half * 4 + row
                        r = (rx, ry, rz)
                        a, b, c = (r[axis] for axis in PATHS[tile])
                        acc[tile, a, b, c] = total[row * 8 : row * 8 + 8, :]

    waits = {}

    def begin(tile):
        axis = PATHS[tile][0]
        ahead, behind = at(axis, 1), at(axis, 3)
        into = first_in
        part = acc.at[tile]
        lo, hi = pl.ds(0, 2), pl.ds(2, 2)
        waits[tile, 1] = [
            send(part.at[2, lo], into.at[tile, 0], ahead),
            send(part.at[2, hi], into.at[tile, 1], behind),
        ]
        waits[tile, 2] = [
            send(part.at[1, hi], into.at[tile, 2], ahead),
            send(part.at[3, lo], into.at[tile, 3], behind),
        ]

    def go_on(tile, step):
        for copy in waits[tile, step]:
            copy.wait_recv()
        if step == 1:
            axis = PATHS[tile][0]
            acc[tile, 1, 0:2] += first_in[tile, 0]
            acc[tile, 3, 2:4] += first_in[tile, 1]
            waits[tile, 2] += [
                send(acc.at[tile, 1, pl.ds(0, 2)], first_in.at[tile, 4], at(axis, 1)),
                send(acc.at[tile, 3, pl.ds(2, 2)], first_in.at[tile, 5], at(axis, 3)),
            ]
        elif step == 2:
            axis = PATHS[tile][1]
            acc[tile, 0, 0:2] += first_in[tile, 3] + first_in[tile, 4]
            acc[tile, 0, 2:4] += first_in[tile, 2] + first_in[tile, 5]
            waits[tile, 3] = [
                send(acc.at[tile, 0, r], second_in.at[tile, r - 1], at(axis, r)) for r in (2, 1, 3)
            ]
        elif step == 3:
            axis = PATHS[tile][2]
            acc[tile, 0, 0] += second_in[tile, 0] + second_in[tile, 1] + second_in[tile, 2]
            waits[tile, 4] = [
                send(acc.at[tile, 0, 0, r], third_in.at[tile, r - 1], at(axis, r)) for r in (2, 1, 3)
            ]
        else:
            half, row = divmod(tile, 4)
            out_ref[row * 8 : row * 8 + 8, half * HALF : (half + 1) * HALF] = (
                acc[tile, 0, 0, 0] + third_in[tile, 0] + third_in[tile, 1] + third_in[tile, 2]
            )

    blocks(0, 0)
    pl.semaphore_wait(barrier, len(greeted))
    look_copy = pltpu.make_async_copy(table, look, look_sem.at[0])
    look_copy.start()
    table_copy = send(table, table_there, partner)
    passed = [pass_on(0, 0)]
    for chunk in range(1, CHUNKS):
        blocks(0, chunk)
        passed.append(pass_on(0, chunk))
    passed_second = []
    for chunk in range(0, 4):
        blocks(1, chunk)
        passed_second.append(pass_on(1, chunk))
    table_copy.wait_recv()
    look_there_copy = pltpu.make_async_copy(table_there, look_there, look_sem.at[1])
    look_there_copy.start()
    look_copy.wait()
    look_there_copy.wait()
    for copy in passed:
        copy.wait_recv()
    assemble(0)
    for tile in range(4):
        begin(tile)
    for chunk in range(4, CHUNKS):
        blocks(1, chunk)
        passed_second.append(pass_on(1, chunk))
    for copy in passed_second:
        copy.wait_recv()
    assemble(1)
    for tile in range(4, 8):
        begin(tile)
    for tile, step in ORDER:
        go_on(tile, step)
    for copy in sent:
        copy.wait_send()


def local(
    density, velocity, pressure, normal, direction, weights, bin_index, group_index, item_count
):
    in_hbm = pl.BlockSpec(memory_space=pltpu.HBM)
    f32, bf16, i32 = jnp.float32, jnp.bfloat16, jnp.int32
    copies = 1 + 2 * CHUNKS + 8 * 12
    return pl.pallas_call(
        kernel,
        out_shape=jax.ShapeDtypeStruct((STEPS, FACES), f32),
        in_specs=[in_hbm] * 9,
        out_specs=pl.BlockSpec(memory_space=pltpu.VMEM),
        scratch_shapes=[
            pltpu.VMEM((STEPS + 2, FACES), f32),
            pltpu.VMEM((3, STEPS + 2, FACES), f32),
            pltpu.VMEM((STEPS + 2, FACES), f32),
            pltpu.VMEM((3, FACES), f32),
            pltpu.SMEM((3, 1, ITEMS), f32),
            pltpu.VMEM((1, ITEMS), i32),
            pltpu.VMEM((1, ITEMS), i32),
            pltpu.SMEM((1, 1), i32),
            pltpu.VMEM((4, STEPS + 2, FACES), f32),
            pltpu.VMEM((6, STEPS, FACES), f32),
            pltpu.VMEM((STEPS, FACES), bf16),
            pltpu.VMEM((ITEMS, STEPS, 3 * FACES), bf16),
            pltpu.VMEM((2, ITEMS, 3 * FACES, HALF), bf16),
            pltpu.VMEM((ITEMS + 1, STEPS, HALF), f32),
            pltpu.VMEM((ITEMS + 1, STEPS, HALF), f32),
            pltpu.VMEM((ITEMS + 1, STEPS, HALF), f32),
            pltpu.VMEM((ITEMS + 1, STEPS, HALF), f32),
            pltpu.VMEM((2, 128), i32),
            pltpu.VMEM((2, 128), i32),
            pltpu.SMEM((2, 128), i32),
            pltpu.SMEM((2, 128), i32),
            pltpu.VMEM((8, 4, 4, 4, 8, 128), f32),
            pltpu.VMEM((8, 6, 2, 4, 8, 128), f32),
            pltpu.VMEM((8, 3, 4, 8, 128), f32),
            pltpu.VMEM((8, 3, 8, 128), f32),
            pltpu.SemaphoreType.DMA((8,)),
            pltpu.SemaphoreType.DMA((2 * CHUNKS,)),
            pltpu.SemaphoreType.DMA((2,)),
            pltpu.SemaphoreType.DMA((copies,)),
            pltpu.SemaphoreType.DMA((copies,)),
        ],
        compiler_params=pltpu.CompilerParams(
            collective_id=0, has_side_effects=True, vmem_limit_bytes=56 * 1024 * 1024
        ),
    )(
        density,
        velocity,
        pressure,
        normal,
        direction.transpose(2, 0, 1),
        weights.reshape(weights.shape[1:]),
        bin_index,
        group_index,
        item_count.reshape(1, 1),
    )


def solution(mesh):
    placed = (
        P(None, ("obs", "face")),
        P(None, None, ("obs", "face")),
        P(None, ("obs", "face")),
        P(None, ("obs", "face")),
        P(("obs", "face"), None, None),
        P(("obs", "face"), None, None, None),
        P(("obs", "face"), None),
        P(("obs", "face"), None),
        P(("obs", "face")),
    )
    return jax.shard_map(
        local, mesh=mesh, in_specs=placed, out_specs=P("face", "obs"), check_vma=False
    )
```
